256 devices in a mesh: ctx: 32 (over y, z_lo, core), section: 8 (over z_hi, x).
Axes of the slice: x: 4, y: 4, z: 8 (z_hi: 2, z_lo: 4; z = z_hi * 4 + z_lo), core: 2. Of those that a mesh axis runs over, the one named last changes fastest.
Arguments:
- queries: bfloat16 [8, 4096, 2560], P('section', 'ctx'), may hold values from -80 to 80
- grad_out: bfloat16 [8, 4096, 2560], P('section', 'ctx'), may hold values from -6 to 6
- keys_values: bfloat16 [2, 4096, 512], P(None, 'ctx'), may hold values from -16 to 16
- doc_ids: int32 [4096], replicated, may hold values from 0 to 7, never falling along the last dimension, each value on 1 to 1024 neighbouring positions
Outputs:
- grad_queries: bfloat16 [8, 4096, 2560], P('section', 'ctx')
- grad_kv: bfloat16 [2, 4096, 512], P(None, ('ctx', 'section'))
The draws below stay inside these ranges and needn't reach their ends.
Inputs may be any that keep to these rules, and one draw needn't show every extreme that they name: `doc_ids`: document numbers never fall along the sequence; a document has at most 1024 tokens.
All inputs are finite; a program needn't handle non-finite values.
Results may differ from the reference program's by a relative error of at most 0.015.
Values may be sent and summed in bfloat16 or wider, within the bound.
No kernel may reach another device: no remote copies, remote signals or barrier semaphores. Data moves between devices by JAX's collectives and lax.ppermute only.
A program may use at most 64 MiB of HBM per device.

```python
import math
import jax
import jax.numpy as jnp
import numpy as np
from jax import lax

HD = 128
KVH = 4
GROUP = 5
TOKENS = 4096
LAYERS = 8
HEADS = 20


def cache_base(key):
    keys = jnp.clip(jax.random.normal(jax.random.fold_in(key, 11), (TOKENS, KVH, HD), jnp.float32), -5.0, 5.0)
    values = jnp.clip(jax.random.normal(jax.random.fold_in(key, 12), (TOKENS, KVH, HD), jnp.float32), -5.0, 5.0)
    return (keys, values)


def draw_keys_values(key, part):
    keys, values = cache_base(key)
    return jnp.stack([keys, values]).reshape(2, TOKENS, KVH * HD).astype(jnp.bfloat16)


def draw_queries(key, part):
    shaped = jnp.clip(jax.random.normal(jax.random.fold_in(key, 13), (LAYERS, TOKENS, KVH, GROUP, HD), jnp.float32), -5.0, 5.0)
    return shaped.reshape(LAYERS, TOKENS, KVH * GROUP * HD).astype(jnp.bfloat16)


def level_of(stream_key, dims, cuts, smallest, top_value):
    loudness = 1.0
    for axis_at, shards_of in cuts:
        steps = jax.random.uniform(jax.random.fold_in(jax.random.fold_in(stream_key, 6), axis_at), (shards_of,), jnp.float32, smallest / len(cuts), top_value / len(cuts))
        loudness = loudness * jnp.repeat(jnp.exp(steps), dims[axis_at] // shards_of).reshape((-1,) + (1,) * (len(dims) - 1 - axis_at))
    return loudness


def split_up(number_of, total, reach, lean):
    portions = [(1 << 20) // math.isqrt(standing ** lean) + 1 for standing in range(2, number_of + 1)]
    spare, holding = total - reach - (number_of - 1), [1] * (number_of - 1)
    while spare > 0:
        free = [i for i in range(number_of - 1) if holding[i] < reach]
        mass, budget = sum([portions[i] for i in free]), spare
        for i in free:
            addition = min(reach - holding[i], max(1, budget * portions[i] // mass), spare)
            holding[i] = holding[i] + addition
            spare = spare - addition
    return np.array([reach] + holding)


def ragged_sizes(stream_key, amount, total, reach, lean):
    if amount == 2:
        one = jax.random.randint(stream_key, (), max(1, total - reach), min(reach, total - 1) + 1)
        return jnp.stack([one, total - one])
    lengths = jnp.asarray(split_up(amount, total, reach, lean), jnp.int32)
    twos = (amount - 1) // 2
    giver, receiver = lengths[1:1 + 2 * twos:2], lengths[2:2 + 2 * twos:2]
    room = jnp.minimum(giver - 1, reach - receiver)
    moved = jax.random.randint(jax.random.fold_in(stream_key, 1), (twos,), 0, 1 << 20) % (room + 1)
    lengths = lengths.at[1:1 + 2 * twos:2].set(giver - moved).at[2:2 + 2 * twos:2].set(receiver + moved)
    return lengths[jax.random.permutation(jax.random.fold_in(stream_key, 2), amount)]


def noise(own_key, dims, spread, limit, split=(), kind=jnp.bfloat16):
    result = jax.random.normal(own_key, dims, jnp.float32) * spread
    if len(split) > 0:
        result = level_of(own_key, dims, split, -0.22, 0.18) * result
    return jnp.clip(result, min=-limit, max=limit).astype(kind)


def setup_inputs(seed: int = 0) -> dict:
    streams_of = jax.random.split(jax.random.key(seed), 5)
    queries = draw_queries(jax.random.fold_in(streams_of[4], 71), 0)
    grad_out = noise(streams_of[1], (LAYERS, TOKENS, HEADS * HD), 1.0, 6.0, ((0, 8), (1, 32)))
    keys_values = draw_keys_values(jax.random.fold_in(streams_of[4], 71), 0)
    doc_ids = jnp.searchsorted(jnp.cumsum(ragged_sizes(streams_of[3], 8, TOKENS, TOKENS // 4, 1)), jnp.arange(TOKENS), side="right").astype(jnp.int32)
    return {"queries": queries, "grad_out": grad_out, "keys_values": keys_values, "doc_ids": doc_ids}


def reference(queries, grad_out, keys_values, doc_ids):
    scale = HD ** -0.5
    keys = keys_values[0].reshape(TOKENS, KVH, HD).astype(jnp.float32)
    values = keys_values[1].reshape(TOKENS, KVH, HD).astype(jnp.float32)
    qblock = min(512, TOKENS)
    nblocks = TOKENS // qblock
    places = jnp.arange(TOKENS, dtype=jnp.int32)

    def one_block(carry, index):
        layer = index // nblocks
        start = (index % nblocks) * qblock
        qrows = lax.dynamic_slice_in_dim(queries[layer], start, qblock, 0).reshape(qblock, KVH, GROUP, HD).astype(jnp.float32)
        grows = lax.dynamic_slice_in_dim(grad_out[layer], start, qblock, 0).reshape(qblock, KVH, GROUP, HD).astype(jnp.float32)
        qplace = start + jnp.arange(qblock, dtype=jnp.int32)
        qdoc = lax.dynamic_slice_in_dim(doc_ids, start, qblock, 0)
        visible = (places[None, :] <= qplace[:, None]) & (doc_ids[None, :] == qdoc[:, None])
        seen = visible[:, None, None, :]
        scores = jnp.einsum("rgnd,kgd->rgnk", qrows, keys) * scale
        scores = jnp.where(seen, scores, -1e30)
        top = jnp.max(scores, axis=-1)
        lse = top + jnp.log(jnp.sum(jnp.exp(scores - top[..., None]), axis=-1))
        weights = jnp.where(seen, jnp.exp(scores - lse[..., None]), 0.0)
        out = jnp.einsum("rgnk,kgd->rgnd", weights, values, precision=lax.Precision.HIGHEST)
        delta = jnp.sum(grows * out, axis=-1)
        prob = weights.astype(jnp.bfloat16).astype(jnp.float32)
        dprob = jnp.einsum("rgnd,kgd->rgnk", grows, values)
        dscore = (prob * (dprob - delta[..., None])).astype(jnp.bfloat16).astype(jnp.float32)
        dquery = (scale * jnp.einsum("rgnk,kgd->rgnd", dscore, keys)).astype(jnp.bfloat16)
        dkeys = scale * jnp.einsum("rgnk,rgnd->kgd", dscore, qrows)
        dvalues = jnp.einsum("rgnk,rgnd->kgd", prob, grows)
        return (carry[0] + dkeys, carry[1] + dvalues), dquery.reshape(qblock, HEADS * HD)

    start_sums = (jnp.zeros((TOKENS, KVH, HD), jnp.float32), jnp.zeros((TOKENS, KVH, HD), jnp.float32))
    sums, dqueries = lax.scan(one_block, start_sums, jnp.arange(LAYERS * nblocks, dtype=jnp.int32))
    grad_queries = dqueries.reshape(LAYERS, TOKENS, HEADS * HD)
    grad_kv = jnp.stack([sums[0], sums[1]]).reshape(2, TOKENS, KVH * HD).astype(jnp.bfloat16)
    return grad_queries, grad_kv
```

```python
import functools, math
import jax, jax.numpy as jnp
from jax import lax
from jax.sharding import PartitionSpec as P
from jax.experimental import pallas as pl
from jax.experimental.pallas import tpu as pltpu
HD=128
TOK=128
def attn_kernel(heads_in, groups, nb, CH, qd_ref, s_in_ref, r_in_ref, bias_ref, dq_ref, ds_out_ref, dr_out_ref,
                k_ref, v_ref, kt_ref, sc_ref, dp_ref, dsb_ref, dk_ref, dv_ref):
    nkeys = nb*TOK
    scale = HD ** -0.5
    c2 = scale*math.log2(math.e)
    for b in range(nb):
        src = s_in_ref if b%2==0 else r_in_ref
        k_ref[b*TOK:(b+1)*TOK,:] = src[b//2,0]
        v_ref[b*TOK:(b+1)*TOK,:] = src[b//2,1]
        kt_ref[:, b*TOK:(b+1)*TOK] = src[b//2,0].T
    dk_ref[...] = jnp.zeros_like(dk_ref)
    dv_ref[...] = jnp.zeros_like(dv_ref)
    def step(p, carry):
        places=[]
        for o in (0,1):
            h = 2*p+o
            l = h//groups
            places.append((l, pl.ds(pl.multiple_of((h-l*groups)*HD,HD),HD)))
        (la,na),(lb,nb_)=places
        qq = jnp.concatenate([qd_ref[la,0,:,na], qd_ref[lb,0,:,nb_]],axis=0)
        dd = jnp.concatenate([qd_ref[la,1,:,na], qd_ref[lb,1,:,nb_]],axis=0)
        nt = (((1,),(1,)),((),()))
        top = jnp.full((8,2*TOK),-3e38,jnp.float32)
        for c in range(0,nkeys,CH):
            s = lax.dot_general(k_ref[c:c+CH,:], qq, nt, preferred_element_type=jnp.float32)
            bias = bias_ref[c:c+CH,:]
            s = s*c2 + jnp.concatenate([bias,bias],axis=1)
            sc_ref[c:c+CH,:] = s
            top = jnp.maximum(top, jnp.max(s.reshape(CH//8,8,2*TOK),axis=0))
        top = jnp.max(top,axis=0,keepdims=True)
        tot = jnp.zeros((8,2*TOK),jnp.float32)
        dl = jnp.zeros((8,2*TOK),jnp.float32)
        for c in range(0,nkeys,CH):
            dp = lax.dot_general(v_ref[c:c+CH,:], dd, nt, preferred_element_type=jnp.float32)
            e = jnp.exp2(sc_ref[c:c+CH,:]-top)
            tot = tot + jnp.sum(e.reshape(CH//8,8,2*TOK),axis=0)
            dl = dl + jnp.sum((e*dp).reshape(CH//8,8,2*TOK),axis=0)
            sc_ref[c:c+CH,:] = e
            dp_ref[c:c+CH,:] = dp
        rec = 1.0/jnp.sum(tot,axis=0,keepdims=True)
        delta = jnp.sum(dl,axis=0,keepdims=True)*rec
        for c in range(0,nkeys,CH):
            prob = (sc_ref[c:c+CH,:]*rec).astype(jnp.bfloat16)
            ds = (prob.astype(jnp.float32)*(dp_ref[c:c+CH,:]-delta)).astype(jnp.bfloat16)
            dsb_ref[c:c+CH,:] = ds
            dv_ref[c:c+CH,:] += jnp.dot(prob, dd, preferred_element_type=jnp.float32)
            dk_ref[c:c+CH,:] += jnp.dot(ds, qq, preferred_element_type=jnp.float32)
        dqt = jnp.dot(kt_ref[...], dsb_ref[...], preferred_element_type=jnp.float32)
        dqq = (dqt.T*scale).astype(jnp.bfloat16)
        dq_ref[la,:,na] = dqq[:TOK]
        dq_ref[lb,:,nb_] = dqq[TOK:]
        return carry
    lax.fori_loop(0, heads_in//2, step, 0)
    for b in range(nb):
        dst = ds_out_ref if b%2==0 else dr_out_ref
        dst[b//2,0] = (dk_ref[b*TOK:(b+1)*TOK,:]*scale).astype(dst.dtype)
        dst[b//2,1] = dv_ref[b*TOK:(b+1)*TOK,:].astype(dst.dtype)

def attn(qd, s_in, r_in, bias, CH=384):
    L=qd.shape[0]; groups=qd.shape[3]//HD
    ns, nr = s_in.shape[0], r_in.shape[0]
    nb=ns+nr; nk=nb*TOK
    body=functools.partial(attn_kernel, L*groups, groups, nb, CH)
    flops=5*2*L*TOK*groups*HD*nk
    vm=pl.BlockSpec(memory_space=pltpu.VMEM)
    return pl.pallas_call(body,
        out_shape=(jax.ShapeDtypeStruct((L,TOK,groups*HD),jnp.bfloat16),
                   jax.ShapeDtypeStruct((ns,2,TOK,HD),jnp.float32),
                   jax.ShapeDtypeStruct((nr,2,TOK,HD),jnp.bfloat16)),
        in_specs=[vm]*4, out_specs=(vm,)*3,
        scratch_shapes=[pltpu.VMEM((nk,HD),jnp.bfloat16),pltpu.VMEM((nk,HD),jnp.bfloat16),pltpu.VMEM((HD,nk),jnp.bfloat16),
            pltpu.VMEM((nk,2*TOK),jnp.float32),pltpu.VMEM((nk,2*TOK),jnp.float32),pltpu.VMEM((nk,2*TOK),jnp.bfloat16),
            pltpu.VMEM((nk,HD),jnp.float32),pltpu.VMEM((nk,HD),jnp.float32)],
        cost_estimate=pl.CostEstimate(flops=flops,bytes_accessed=4*1024*1024,transcendentals=L*TOK*groups*nk),
        compiler_params=pltpu.CompilerParams(vmem_limit_bytes=32*1024*1024),
        name="attn_bwd")(qd,s_in,r_in,bias)


def chip_back(value, chips):
    count = lax.axis_size("ctx")
    steps = 2 * chips
    first, last = (max(0, -steps), min(count, count - steps))
    return lax.ppermute(value, "ctx", [(s, s + steps) for s in range(first, last)])


def other_core(value):
    return lax.ppermute(value, "ctx", [(s, s ^ 1) for s in range(lax.axis_size("ctx"))])


def body(queries, grad_out, keys_values, doc_ids):
    layers, tok_rows, width = queries.shape
    kv_width = keys_values.shape[2]
    heads_kv = kv_width // HD
    part = width // heads_kv
    count = lax.axis_size("ctx")
    sections = lax.axis_size("section")
    chips = count // 8
    place = lax.axis_index("ctx")
    core = place % 2
    head = lax.axis_index("section") % heads_kv
    xgroups = [[g + i for i in range(heads_kv)] for g in range(0, sections, heads_kv)]

    qd = jnp.stack([queries[0], grad_out[0]]).reshape(2, tok_rows, heads_kv, part)
    qd = qd.transpose(2, 0, 1, 3)
    qd = lax.all_to_all(qd, "section", 0, 0, axis_index_groups=xgroups, tiled=True)

    own = lax.dynamic_slice_in_dim(keys_values, head * HD, HD, 2)
    same = jnp.stack([chip_back(own, d) for d in range(chips, 0, -1)] + [own])
    cross = other_core(lax.dynamic_slice_in_dim(same, 1 - core, chips, 0))

    span = 2 * chips + 1
    total = span * tok_rows
    first = place * tok_rows
    qdoc = lax.dynamic_slice_in_dim(doc_ids, first, tok_rows, 0)
    padded = jnp.concatenate([jnp.full((total - tok_rows,), -1, jnp.int32), doc_ids])
    kdoc = lax.dynamic_slice_in_dim(padded, first, total, 0)
    kat = jnp.arange(total, dtype=jnp.int32) - (total - tok_rows)
    qat = jnp.arange(tok_rows, dtype=jnp.int32)
    seen = (kat[:, None] <= qat[None, :]) & (kdoc[:, None] == qdoc[None, :])
    bias = jnp.where(seen, 0.0, -1e30).astype(jnp.float32)

    dq, dsame, dcross = attn(qd, same, cross, bias)

    arrived = other_core(dcross).astype(jnp.float32)
    zero = jnp.zeros((1,) + arrived.shape[1:], jnp.float32)
    dsame = dsame + jnp.where(
        core == 1, jnp.concatenate([arrived, zero]), jnp.concatenate([zero, arrived])
    )
    grad = dsame[chips]
    for d in range(chips, 0, -1):
        grad = grad + chip_back(dsame[chips - d].astype(jnp.bfloat16), -d).astype(jnp.float32)

    dq = lax.all_to_all(dq, "section", 0, 0, axis_index_groups=xgroups, tiled=True)
    grad_queries = dq.transpose(1, 0, 2).reshape(1, tok_rows, width)

    rows = tok_rows // sections
    pieces = grad.astype(jnp.bfloat16).reshape(2, sections, rows, HD).transpose(1, 0, 2, 3)
    got = lax.all_to_all(pieces, "section", 0, 0, tiled=True).astype(jnp.float32)
    got = got.reshape(sections // heads_kv, heads_kv, 2, rows, HD).sum(axis=0)
    grad_kv = got.transpose(1, 2, 0, 3).reshape(2, rows, kv_width).astype(jnp.bfloat16)
    return (grad_queries, grad_kv)


def solution(mesh):
    return jax.shard_map(
        body,
        mesh=mesh,
        in_specs=(P("section", "ctx", None), P("section", "ctx", None), P(None, "ctx", None), P()),
        out_specs=(P("section", "ctx", None), P(None, ("ctx", "section"), None)),
        check_vma=False,
    )
```

```python
import functools, math
import jax, jax.numpy as jnp
from jax import lax
from jax.sharding import PartitionSpec as P
from jax.experimental import pallas as pl
from jax.experimental.pallas import tpu as pltpu


HD = 128
LINE = 4


def window_slots():
    core, chip = lax.axis_index("core"), lax.axis_index("z")
    turn = [lax.rem(i + LINE - chip, LINE) for i in range(LINE)]
    same = [2 * t for t in turn]
    cross = [lax.rem(2 * t + 1 + 6 * core, 2 * LINE) for t in turn]
    return chip, same, cross


def attn_kernel(slots, chunk, *refs):
    pieces, refs = refs[:slots], refs[slots:]
    line_ref, prev_ref, own_ref, cross_ref, bias_ref, *refs = refs
    dq_out, refs = refs[:slots], refs[slots:]
    dline, down, dcross, *refs = refs
    qd_ref, dq_ref, k_ref, v_ref, kt_ref, sc_ref, dp_ref, dsb_ref, dk_ref, dv_ref = refs
    tok, part = dq_out[0].shape
    groups = part // HD
    nkeys = k_ref.shape[0]
    scale = HD ** (-0.5)
    c2 = scale * math.log2(math.e)
    _, same_at, cross_at = window_slots()
    own_at = 2 * LINE

    def rows(w):
        return pl.ds(pl.multiple_of(w * tok, tok), tok)

    def put(w, kpart, vpart):
        k_ref[rows(w), :] = kpart
        v_ref[rows(w), :] = vpart
        kt_ref[:, rows(w)] = kpart.T

    for s in range(slots):
        qd_ref[s] = pieces[s][...]
    for i in range(LINE):
        put(same_at[i], line_ref[i, 0], line_ref[i, 1])
        put(cross_at[i], cross_ref[i, 0], cross_ref[i, 1])
    put(0, prev_ref[0], prev_ref[1])
    put(own_at, own_ref[0], own_ref[1])
    dk_ref[...] = jnp.zeros_like(dk_ref)
    dv_ref[...] = jnp.zeros_like(dv_ref)
    nt = (((1,), (1,)), ((), ()))
    wide = 2 * tok

    def folded(x):
        return x.reshape(chunk // 8, 8, wide)

    def step(p, carry):
        places = []
        for o in (0, 1):
            h = 2 * p + o
            slot = h // groups
            places.append((slot, pl.ds(pl.multiple_of((h - slot * groups) * HD, HD), HD)))
        (sa, na), (sb, nb_) = places
        qq = jnp.concatenate([qd_ref[sa, 0, :, na], qd_ref[sb, 0, :, nb_]], axis=0)
        dd = jnp.concatenate([qd_ref[sa, 1, :, na], qd_ref[sb, 1, :, nb_]], axis=0)
        top = jnp.full((8, wide), -3e38, jnp.float32)
        for c in range(0, nkeys, chunk):
            s = lax.dot_general(k_ref[c : c + chunk, :], qq, nt, preferred_element_type=jnp.float32)
            bias = bias_ref[c : c + chunk, :]
            s = s * c2 + jnp.concatenate([bias, bias], axis=1)
            sc_ref[c : c + chunk, :] = s
            top = jnp.maximum(top, jnp.max(folded(s), axis=0))
        top = jnp.max(top, axis=0, keepdims=True)
        tot = jnp.zeros((8, wide), jnp.float32)
        dl = jnp.zeros((8, wide), jnp.float32)
        for c in range(0, nkeys, chunk):
            dp = lax.dot_general(v_ref[c : c + chunk, :], dd, nt, preferred_element_type=jnp.float32)
            e = jnp.exp2(sc_ref[c : c + chunk, :] - top)
            tot = tot + jnp.sum(folded(e), axis=0)
            dl = dl + jnp.sum(folded(e * dp), axis=0)
            sc_ref[c : c + chunk, :] = e
            dp_ref[c : c + chunk, :] = dp
        rec = 1.0 / jnp.sum(tot, axis=0, keepdims=True)
        delta = jnp.sum(dl, axis=0, keepdims=True) * rec
        for c in range(0, nkeys, chunk):
            prob = (sc_ref[c : c + chunk, :] * rec).astype(jnp.bfloat16)
            ds = (prob.astype(jnp.float32) * (dp_ref[c : c + chunk, :] - delta)).astype(jnp.bfloat16)
            dsb_ref[c : c + chunk, :] = ds
            dv_ref[c : c + chunk, :] += jnp.dot(prob, dd, preferred_element_type=jnp.float32)
            dk_ref[c : c + chunk, :] += jnp.dot(ds, qq, preferred_element_type=jnp.float32)
        dqt = jnp.dot(kt_ref[...], dsb_ref[...], preferred_element_type=jnp.float32)
        dqq = (dqt.T * scale).astype(jnp.bfloat16)
        dq_ref[sa, :, na] = dqq[:tok]
        dq_ref[sb, :, nb_] = dqq[tok:]
        return carry

    lax.fori_loop(0, slots * groups // 2, step, 0)
    for s in range(slots):
        dq_out[s][...] = dq_ref[s]

    def grads(dst, w):
        dst[0] = (dk_ref[rows(w), :] * scale).astype(dst.dtype)
        dst[1] = dv_ref[rows(w), :].astype(dst.dtype)

    for i in range(LINE):
        grads(dline.at[i], same_at[i])
        grads(dcross.at[i], cross_at[i])
    grads(down, own_at)


def attn_parts(pieces, line, prev, own, cross, bias, chunk=384):
    slots = len(pieces)
    tok, part = pieces[0].shape[1:]
    nk = bias.shape[0]
    vm = pl.BlockSpec(memory_space=pltpu.VMEM)
    bf, f32 = jnp.bfloat16, jnp.float32
    return pl.pallas_call(
        functools.partial(attn_kernel, slots, chunk),
        out_shape=(
            *[jax.ShapeDtypeStruct((tok, part), bf) for _ in range(slots)],
            jax.ShapeDtypeStruct(line.shape, f32),
            jax.ShapeDtypeStruct(own.shape, f32),
            jax.ShapeDtypeStruct(cross.shape, bf),
        ),
        in_specs=[vm] * (slots + 5),
        out_specs=(vm,) * (slots + 3),
        scratch_shapes=[
            pltpu.VMEM((slots, 2, tok, part), bf),
            pltpu.VMEM((slots, tok, part), bf),
            pltpu.VMEM((nk, HD), bf),
            pltpu.VMEM((nk, HD), bf),
            pltpu.VMEM((HD, nk), bf),
            pltpu.VMEM((nk, 2 * tok), f32),
            pltpu.VMEM((nk, 2 * tok), f32),
            pltpu.VMEM((nk, 2 * tok), bf),
            pltpu.VMEM((nk, HD), f32),
            pltpu.VMEM((nk, HD), f32),
        ],
        cost_estimate=pl.CostEstimate(
            flops=10 * slots * tok * part * nk,
            bytes_accessed=4 * 1024 * 1024,
            transcendentals=slots * tok * part // HD * nk,
        ),
        compiler_params=pltpu.CompilerParams(vmem_limit_bytes=32 * 1024 * 1024),
        name="attn_bwd",
    )(*pieces, line, prev, own, cross, bias)


def join_kernel(sign, *refs):
    *pieces, out_ref, sems = refs
    count, part = len(pieces), pieces[0].shape[-1]
    head = lax.axis_index("x")
    copies = []
    for n, piece in enumerate(pieces):
        at = lax.rem(head + (count + sign * n) % count, count) * part
        copies.append(
            pltpu.make_async_copy(piece, out_ref.at[:, pl.ds(pl.multiple_of(at, HD), part)], sems.at[n])
        )
    for c in copies:
        c.start()
    for c in copies:
        c.wait()


def joined(pieces, sign):
    rows, part = pieces[0].shape
    vm = pl.BlockSpec(memory_space=pltpu.VMEM)
    return pl.pallas_call(
        functools.partial(join_kernel, sign),
        out_shape=jax.ShapeDtypeStruct((rows, len(pieces) * part), pieces[0].dtype),
        in_specs=[vm] * len(pieces),
        out_specs=pl.BlockSpec(memory_space=pl.ANY),
        scratch_shapes=[pltpu.SemaphoreType.DMA((len(pieces),))],
        compiler_params=pltpu.CompilerParams(vmem_limit_bytes=2 * 1024 * 1024),
        name="join_heads",
    )(*pieces)


def shifted(value, axis, steps, ring):
    count = lax.axis_size(axis)
    pairs = [(i, i + steps) for i in range(count)]
    pairs = [(i, j % count) for i, j in pairs if ring or 0 <= j < count]
    return lax.ppermute(value, axis, pairs)


def exchanged(value, axes):
    return lax.all_to_all(value, axes, 0, 0, tiled=True)


def chosen(which, options):
    out = options[0]
    for n, option in enumerate(options[1:], 1):
        out = jnp.where(which == n, option, out)
    return out


def body(queries, grad_out, keys_values, doc_ids):
    _, tok_rows, width = queries.shape
    kv_width = keys_values.shape[2]
    ring = lax.axis_size("x")
    part = width // ring
    core, chip, head = [lax.axis_index(a) for a in ("core", "z", "x")]
    place = (lax.axis_index("y") * LINE + chip) * 2 + core
    bf, f32 = jnp.bfloat16, jnp.float32
    chips = jnp.arange(LINE, dtype=jnp.int32).reshape(LINE, 1, 1, 1)

    def cut(arrays, k):
        at = lax.rem(head + k, ring) * part
        return jnp.stack([lax.dynamic_slice_in_dim(a[0], at, part, 1) for a in arrays])

    far = cut((queries, grad_out), 2)
    pieces = {2: shifted(far, "x", 2, True)}
    own = chosen(head, jnp.split(keys_values, ring, axis=2))
    prev = shifted(own, "y", 1, False)
    near = (queries, grad_out)
    for k in (1, 3):
        pieces[k] = shifted(cut(near, k), "x", k, True)
    pieces = [cut(near, 0), pieces[1], pieces[2], pieces[3]]
    line = exchanged(jnp.where(chips > chip, own[None], prev[None]), "z")
    cross = jnp.where(chips == chip, jnp.where(core == 1, prev, own)[None], line)
    cross = shifted(cross, "core", 1, True)

    total = (2 * LINE + 1) * tok_rows
    first = place * tok_rows
    qdoc = lax.dynamic_slice_in_dim(doc_ids, first, tok_rows, 0)
    padded = jnp.concatenate([jnp.full((total - tok_rows,), -1, jnp.int32), doc_ids])
    kdoc = lax.dynamic_slice_in_dim(padded, first, total, 0)
    kat = jnp.arange(total, dtype=jnp.int32) - (total - tok_rows)
    qat = jnp.arange(tok_rows, dtype=jnp.int32)
    seen = (kat[:, None] <= qat[None, :]) & (kdoc[:, None] == qdoc[None, :])
    bias = jnp.where(seen, 0.0, -1e30).astype(f32)

    *dq, dline, down, dcross = attn_parts(pieces, line, prev, own, cross, bias)

    arrived = shifted(dcross, "core", 1, True).astype(f32)
    dline = dline + jnp.where((chips != chip) | (core == 1), arrived, 0.0)
    later = shifted(jnp.where(chips >= chip, dline, 0.0).astype(bf), "y", -1, False)
    parts = [dq[0]] + [shifted(dq[k], "x", -k, True) for k in range(1, ring)]

    here = down[None] + jnp.where(core == 0, arrived, 0.0)
    later = later.astype(f32) + jnp.where(chips == chip, here, 0.0)
    grad = jnp.where(chips < chip, dline, later).astype(bf)
    sections = lax.axis_size("h") * ring
    rows = tok_rows // sections
    grad = grad.reshape(LINE, 2, sections, rows, HD).transpose(0, 2, 1, 3, 4)
    grad = exchanged(grad.reshape(LINE * sections, 2, rows, HD), ("z", "h", "x"))
    grad = grad.astype(f32).reshape(LINE * lax.axis_size("h"), ring, 2, rows, HD).sum(axis=0)
    grad_kv = grad.astype(bf).transpose(1, 2, 0, 3).reshape(2, rows, kv_width)
    grad_queries = joined(parts, 1).reshape(1, tok_rows, width)
    return (grad_queries, grad_kv)


def solution(mesh):
    names = ("y", "z", "core", "h", "x")
    fine = jax.sharding.Mesh(mesh.devices.reshape(-1, LINE, 2, 2, 4), names)
    ctx, section = names[:3], names[3:]
    return jax.shard_map(
        body,
        mesh=fine,
        in_specs=(P(section, ctx, None), P(section, ctx, None), P(None, ctx, None), P()),
        out_specs=(P(section, ctx, None), P(None, ctx + section, None)),
        check_vma=False,
    )
```

```python
import functools, math
import jax, jax.numpy as jnp
from jax import lax
from jax.sharding import PartitionSpec as P
from jax.experimental import pallas as pl
from jax.experimental.pallas import tpu as pltpu


HD = 128
LINE = 4


def window_slots():
    core, chip = lax.axis_index("core"), lax.axis_index("z")
    turn = [lax.rem(i + LINE - chip, LINE) for i in range(LINE)]
    same = [2 * t for t in turn]
    cross = [lax.rem(2 * t + 1 + 6 * core, 2 * LINE) for t in turn]
    return chip, same, cross


def head_places(pair, groups):
    places = []
    for h in (2 * pair, 2 * pair + 1):
        slot = h // groups
        places.append((slot, pl.ds(pl.multiple_of((h - slot * groups) * HD, HD), HD)))
    return places


def attn_kernel(slots, chunk, *refs):
    pieces, refs = refs[:slots], refs[slots:]
    line_ref, prev_ref, own_ref, cross_ref, bias_ref, *refs = refs
    ds_ref, kt_ref, dline, down, dcross, *refs = refs
    qd_ref, k_ref, v_ref, dk_ref, dv_ref, *pairs = refs
    tok, part = pieces[0].shape[1:]
    groups = part // HD
    nkeys = k_ref.shape[0]
    scale = HD ** (-0.5)
    c2 = scale * math.log2(math.e)
    _, same_at, cross_at = window_slots()
    own_at = 2 * LINE

    def rows(w):
        return pl.ds(pl.multiple_of(w * tok, tok), tok)

    def put(w, kpart, vpart):
        k_ref[rows(w), :] = kpart
        v_ref[rows(w), :] = vpart
        kt_ref[:, rows(w)] = kpart.T

    for s in range(slots):
        qd_ref[s] = pieces[s][...]
    for i in range(LINE):
        put(same_at[i], line_ref[i, 0], line_ref[i, 1])
        put(cross_at[i], cross_ref[i, 0], cross_ref[i, 1])
    put(0, prev_ref[0], prev_ref[1])
    put(own_at, own_ref[0], own_ref[1])
    dk_ref[...] = jnp.zeros_like(dk_ref)
    dv_ref[...] = jnp.zeros_like(dv_ref)
    nt = (((1,), (1,)), ((), ()))
    wide = 2 * tok

    def folded(x):
        return x.reshape(chunk // 8, 8, wide)

    def one(p, sc_ref, dp_ref):
        places = head_places(p, groups)
        (sa, na), (sb, nb_) = places
        qq = jnp.concatenate([qd_ref[sa, 0, :, na], qd_ref[sb, 0, :, nb_]], axis=0)
        dd = jnp.concatenate([qd_ref[sa, 1, :, na], qd_ref[sb, 1, :, nb_]], axis=0)
        top = jnp.full((8, wide), -3e38, jnp.float32)
        for c in range(0, nkeys, chunk):
            s = lax.dot_general(k_ref[c : c + chunk, :], qq, nt, preferred_element_type=jnp.float32)
            bias = bias_ref[c : c + chunk, :]
            s = s * c2 + jnp.concatenate([bias, bias], axis=1)
            sc_ref[c : c + chunk, :] = s
            top = jnp.maximum(top, jnp.max(folded(s), axis=0))
        top = jnp.max(top, axis=0, keepdims=True)
        tot = jnp.zeros((8, wide), jnp.float32)
        dl = jnp.zeros((8, wide), jnp.float32)
        for c in range(0, nkeys, chunk):
            dp = lax.dot_general(v_ref[c : c + chunk, :], dd, nt, preferred_element_type=jnp.float32)
            e = jnp.exp2(sc_ref[c : c + chunk, :] - top)
            tot = tot + jnp.sum(folded(e), axis=0)
            dl = dl + jnp.sum(folded(e * dp), axis=0)
            sc_ref[c : c + chunk, :] = e
            dp_ref[c : c + chunk, :] = dp
        rec = 1.0 / jnp.sum(tot, axis=0, keepdims=True)
        delta = jnp.sum(dl, axis=0, keepdims=True) * rec
        for c in range(0, nkeys, chunk):
            prob = (sc_ref[c : c + chunk, :] * rec).astype(jnp.bfloat16)
            ds = (prob.astype(jnp.float32) * (dp_ref[c : c + chunk, :] - delta)).astype(jnp.bfloat16)
            ds_ref[p, c : c + chunk, :] = ds
            dv_ref[c : c + chunk, :] += jnp.dot(prob, dd, preferred_element_type=jnp.float32)
            dk_ref[c : c + chunk, :] += jnp.dot(ds, qq, preferred_element_type=jnp.float32)

    def step(t, carry):
        for u in range(2):
            one(2 * t + u, pairs[2 * u], pairs[2 * u + 1])
        return carry

    lax.fori_loop(0, slots * groups // 4, step, 0)

    def grads(dst, w):
        block = (dst.shape[0], dst.shape[2], HD)
        dst[:, 0] = (dk_ref[rows(w), :] * scale).astype(dst.dtype).reshape(block)
        dst[:, 1] = dv_ref[rows(w), :].astype(dst.dtype).reshape(block)

    for i in range(LINE):
        grads(dline.at[i], same_at[i])
        grads(dcross.at[i], cross_at[i])
    grads(down, own_at)


def attn_parts(pieces, line, prev, own, cross, bias, sections, chunk=384):
    slots = len(pieces)
    tok, part = pieces[0].shape[1:]
    nk = bias.shape[0]
    block = (sections, 2, tok // sections, HD)
    vm = pl.BlockSpec(memory_space=pltpu.VMEM)
    bf, f32 = jnp.bfloat16, jnp.float32
    return pl.pallas_call(
        functools.partial(attn_kernel, slots, chunk),
        out_shape=(
            jax.ShapeDtypeStruct((slots * part // HD // 2, nk, 2 * tok), bf),
            jax.ShapeDtypeStruct((HD, nk), bf),
            jax.ShapeDtypeStruct((LINE,) + block, f32),
            jax.ShapeDtypeStruct(block, f32),
            jax.ShapeDtypeStruct((LINE,) + block, bf),
        ),
        in_specs=[vm] * (slots + 5),
        out_specs=(vm,) * 5,
        scratch_shapes=[
            pltpu.VMEM((slots, 2, tok, part), bf),
            pltpu.VMEM((nk, HD), bf),
            pltpu.VMEM((nk, HD), bf),
            pltpu.VMEM((nk, HD), f32),
            pltpu.VMEM((nk, HD), f32),
            *[pltpu.VMEM((nk, 2 * tok), f32) for _ in range(4)],
        ],
        cost_estimate=pl.CostEstimate(
            flops=8 * slots * tok * part * nk,
            bytes_accessed=4 * 1024 * 1024,
            transcendentals=slots * tok * part // HD * nk,
        ),
        compiler_params=pltpu.CompilerParams(vmem_limit_bytes=24 * 1024 * 1024),
        name="attn_bwd",
    )(*pieces, line, prev, own, cross, bias)


def dq_kernel(slots, ds_ref, kt_ref, *refs):
    dq_out, dq_ref = refs[:slots], refs[slots]
    tok, part = dq_out[0].shape
    scale = HD ** (-0.5)

    def step(t, carry):
        for u in range(2):
            p = 2 * t + u
            dqt = jnp.dot(kt_ref[...], ds_ref[p], preferred_element_type=jnp.float32)
            dqq = (dqt.T * scale).astype(jnp.bfloat16)
            for o, (slot, n) in enumerate(head_places(p, part // HD)):
                dq_ref[slot, :, n] = dqq[o * tok : (o + 1) * tok]
        return carry

    lax.fori_loop(0, ds_ref.shape[0] // 2, step, 0)
    for s in range(slots):
        dq_out[s][...] = dq_ref[s]


def dq_parts(ds, kt, slots, tok, part):
    vm = pl.BlockSpec(memory_space=pltpu.VMEM)
    bf = jnp.bfloat16
    return pl.pallas_call(
        functools.partial(dq_kernel, slots),
        out_shape=tuple(jax.ShapeDtypeStruct((tok, part), bf) for _ in range(slots)),
        in_specs=[vm] * 2,
        out_specs=(vm,) * slots,
        scratch_shapes=[pltpu.VMEM((slots, tok, part), bf)],
        cost_estimate=pl.CostEstimate(
            flops=2 * ds.size * HD, bytes_accessed=2 * ds.size, transcendentals=0
        ),
        compiler_params=pltpu.CompilerParams(vmem_limit_bytes=12 * 1024 * 1024),
        name="attn_dq",
    )(ds, kt)


def join_kernel(sign, *refs):
    *pieces, out_ref, sems = refs
    count, part = len(pieces), pieces[0].shape[-1]
    head = lax.axis_index("x")
    copies = []
    for n, piece in enumerate(pieces):
        at = lax.rem(head + (count + sign * n) % count, count) * part
        copies.append(
            pltpu.make_async_copy(piece, out_ref.at[:, pl.ds(pl.multiple_of(at, HD), part)], sems.at[n])
        )
    for c in copies:
        c.start()
    for c in copies:
        c.wait()


def joined(pieces, sign):
    rows, part = pieces[0].shape
    vm = pl.BlockSpec(memory_space=pltpu.VMEM)
    return pl.pallas_call(
        functools.partial(join_kernel, sign),
        out_shape=jax.ShapeDtypeStruct((rows, len(pieces) * part), pieces[0].dtype),
        in_specs=[vm] * len(pieces),
        out_specs=pl.BlockSpec(memory_space=pl.ANY),
        scratch_shapes=[pltpu.SemaphoreType.DMA((len(pieces),))],
        compiler_params=pltpu.CompilerParams(vmem_limit_bytes=2 * 1024 * 1024),
        name="join_heads",
    )(*pieces)


def shifted(value, axis, steps, ring):
    count = lax.axis_size(axis)
    pairs = [(i, i + steps) for i in range(count)]
    pairs = [(i, j % count) for i, j in pairs if ring or 0 <= j < count]
    return lax.ppermute(value, axis, pairs)


def exchanged(value, axes):
    return lax.all_to_all(value, axes, 0, 0, tiled=True)


def chosen(which, options):
    out = options[0]
    for n, option in enumerate(options[1:], 1):
        out = jnp.where(which == n, option, out)
    return out


def body(queries, grad_out, keys_values, doc_ids):
    _, tok_rows, width = queries.shape
    kv_width = keys_values.shape[2]
    ring = lax.axis_size("x")
    part = width // ring
    core, chip, head = [lax.axis_index(a) for a in ("core", "z", "x")]
    place = (lax.axis_index("y") * LINE + chip) * 2 + core
    bf, f32 = jnp.bfloat16, jnp.float32
    chips = jnp.arange(LINE, dtype=jnp.int32).reshape(LINE, 1, 1, 1)

    def cut(arrays, k):
        at = lax.rem(head + k, ring) * part
        return jnp.stack([lax.dynamic_slice_in_dim(a[0], at, part, 1) for a in arrays])

    far = cut((queries, grad_out), 2)
    pieces = {2: shifted(far, "x", 2, True)}
    own = chosen(head, jnp.split(keys_values, ring, axis=2))
    prev = shifted(own, "y", 1, False)
    near = (queries, grad_out)
    for k in (1, 3):
        pieces[k] = shifted(cut(near, k), "x", k, True)
    pieces = [cut(near, 0), pieces[1], pieces[2], pieces[3]]
    line = exchanged(jnp.where(chips > chip, own[None], prev[None]), "z")
    cross = jnp.where(chips == chip, jnp.where(core == 1, prev, own)[None], line)
    cross = shifted(cross, "core", 1, True)

    total = (2 * LINE + 1) * tok_rows
    first = place * tok_rows
    qdoc = lax.dynamic_slice_in_dim(doc_ids, first, tok_rows, 0)
    padded = jnp.concatenate([jnp.full((total - tok_rows,), -1, jnp.int32), doc_ids])
    kdoc = lax.dynamic_slice_in_dim(padded, first, total, 0)
    kat = jnp.arange(total, dtype=jnp.int32) - (total - tok_rows)
    qat = jnp.arange(tok_rows, dtype=jnp.int32)
    seen = (kat[:, None] <= qat[None, :]) & (kdoc[:, None] == qdoc[None, :])
    bias = jnp.where(seen, 0.0, -1e30).astype(f32)

    sections = lax.axis_size("h") * ring
    ds, kt, dline, down, dcross = attn_parts(pieces, line, prev, own, cross, bias, sections)

    arrived = shifted(dcross, "core", 1, True).astype(f32)
    chips = chips[..., None]
    dline = dline + jnp.where((chips != chip) | (core == 1), arrived, 0.0)
    later = shifted(jnp.where(chips >= chip, dline, 0.0).astype(bf), "y", -1, False)
    dq = dq_parts(ds, kt, ring, tok_rows, part)
    parts = [dq[0]] + [shifted(dq[k], "x", -k, True) for k in range(1, ring)]

    here = down[None] + jnp.where(core == 1, 0.0, arrived)
    later = later.astype(f32) + jnp.where(chips == chip, here, 0.0)
    grad = jnp.where(chips < chip, dline, later).astype(bf)
    rows = tok_rows // sections
    grad = exchanged(grad.reshape(LINE * sections, 2, rows, HD), ("z", "h", "x"))
    grad = grad.astype(f32).reshape(LINE * lax.axis_size("h"), ring, 2, rows, HD).sum(axis=0)
    grad_kv = grad.astype(bf).transpose(1, 2, 0, 3).reshape(2, rows, kv_width)
    grad_queries = joined(parts, 1).reshape(1, tok_rows, width)
    return (grad_queries, grad_kv)


def solution(mesh):
    names = ("y", "z", "core", "h", "x")
    fine = jax.sharding.Mesh(mesh.devices.reshape(-1, LINE, 2, 2, 4), names)
    ctx, section = names[:3], names[3:]
    return jax.shard_map(
        body,
        mesh=fine,
        in_specs=(P(section, ctx, None), P(section, ctx, None), P(None, ctx, None), P()),
        out_specs=(P(section, ctx, None), P(None, ctx + section, None)),
        check_vma=False,
    )
```

```python
import functools, math
import jax, jax.numpy as jnp
from jax import lax
from jax.sharding import PartitionSpec as P
from jax.experimental import pallas as pl
from jax.experimental.pallas import tpu as pltpu


HD = 128
LINE = 4


def window_slots():
    core, chip = lax.axis_index("core"), lax.axis_index("z")
    turn = [lax.rem(i + LINE - chip, LINE) for i in range(LINE)]
    same = [2 * t for t in turn]
    cross = [lax.rem(2 * t + 1 + 6 * core, 2 * LINE) for t in turn]
    return chip, same, cross


def head_places(pair, groups):
    places = []
    for h in (2 * pair, 2 * pair + 1):
        slot = h // groups
        places.append((slot, pl.ds(pl.multiple_of((h - slot * groups) * HD, HD), HD)))
    return places


def attn_kernel(slots, chunk, *refs):
    pieces, refs = refs[:slots], refs[slots:]
    line_ref, prev_ref, own_ref, cross_ref, bias_ref, *refs = refs
    ds_ref, kt_ref, dline, down, dcross, *refs = refs
    qd_ref, k_ref, v_ref, dk_ref, dv_ref, *pairs = refs
    tok, part = pieces[0].shape[1:]
    groups = part // HD
    nkeys = k_ref.shape[0]
    scale = HD ** (-0.5)
    c2 = scale * math.log2(math.e)
    _, same_at, cross_at = window_slots()
    own_at = 2 * LINE

    def rows(w):
        return pl.ds(pl.multiple_of(w * tok, tok), tok)

    def put(w, kpart, vpart):
        k_ref[rows(w), :] = kpart
        v_ref[rows(w), :] = vpart
        kt_ref[:, rows(w)] = kpart.T

    for s in range(slots):
        qd_ref[s] = pieces[s][...]
    for i in range(LINE):
        put(same_at[i], line_ref[i, 0], line_ref[i, 1])
        put(cross_at[i], cross_ref[i, 0], cross_ref[i, 1])
    put(0, prev_ref[0], prev_ref[1])
    put(own_at, own_ref[0], own_ref[1])
    dk_ref[...] = jnp.zeros_like(dk_ref)
    dv_ref[...] = jnp.zeros_like(dv_ref)
    nt = (((1,), (1,)), ((), ()))
    wide = 2 * tok

    def folded(x):
        return x.reshape(chunk // 8, 8, wide)

    chunks = range(0, nkeys, chunk)

    class Pair:
        def __init__(self, p, sc_ref, dp_ref):
            self.p, self.sc_ref, self.dp_ref = p, sc_ref, dp_ref
            places = head_places(p, groups)
            self.qq = jnp.concatenate([qd_ref[slot, 0, :, n] for slot, n in places], axis=0)
            self.dd = jnp.concatenate([qd_ref[slot, 1, :, n] for slot, n in places], axis=0)
            self.top = jnp.full((8, wide), -3e38, jnp.float32)
            self.tot = jnp.zeros((8, wide), jnp.float32)
            self.dl = jnp.zeros((8, wide), jnp.float32)

        def scores(self, c):
            s = lax.dot_general(k_ref[c : c + chunk, :], self.qq, nt, preferred_element_type=jnp.float32)
            bias = bias_ref[c : c + chunk, :]
            s = s * c2 + jnp.concatenate([bias, bias], axis=1)
            self.sc_ref[c : c + chunk, :] = s
            self.top = jnp.maximum(self.top, jnp.max(folded(s), axis=0))

        def scored(self):
            self.top = jnp.max(self.top, axis=0, keepdims=True)

        def sums(self, c):
            dp = lax.dot_general(v_ref[c : c + chunk, :], self.dd, nt, preferred_element_type=jnp.float32)
            e = jnp.exp2(self.sc_ref[c : c + chunk, :] - self.top)
            self.tot = self.tot + jnp.sum(folded(e), axis=0)
            self.dl = self.dl + jnp.sum(folded(e * dp), axis=0)
            self.sc_ref[c : c + chunk, :] = e
            self.dp_ref[c : c + chunk, :] = dp

        def summed(self):
            self.rec = 1.0 / jnp.sum(self.tot, axis=0, keepdims=True)
            self.delta = jnp.sum(self.dl, axis=0, keepdims=True) * self.rec

        def grads(self, c):
            prob = (self.sc_ref[c : c + chunk, :] * self.rec).astype(jnp.bfloat16)
            ds = prob.astype(jnp.float32) * (self.dp_ref[c : c + chunk, :] - self.delta)
            ds = ds.astype(jnp.bfloat16)
            ds_ref[self.p, c : c + chunk, :] = ds
            dv_ref[c : c + chunk, :] += jnp.dot(prob, self.dd, preferred_element_type=jnp.float32)
            dk_ref[c : c + chunk, :] += jnp.dot(ds, self.qq, preferred_element_type=jnp.float32)

    def step(t, carry):
        one, two = [Pair(2 * t + u, *pairs[2 * u : 2 * u + 2]) for u in (0, 1)]
        for c in chunks:
            one.scores(c)
        one.scored()
        for c in chunks:
            one.sums(c)
            two.scores(c)
        one.summed()
        two.scored()
        for c in chunks:
            one.grads(c)
            two.sums(c)
        two.summed()
        for c in chunks:
            two.grads(c)
        return carry

    lax.fori_loop(0, slots * groups // 4, step, 0)

    def grads(dst, w):
        block = (dst.shape[0], dst.shape[2], HD)
        dst[:, 0] = (dk_ref[rows(w), :] * scale).astype(dst.dtype).reshape(block)
        dst[:, 1] = dv_ref[rows(w), :].astype(dst.dtype).reshape(block)

    for i in range(LINE):
        grads(dline.at[i], same_at[i])
        grads(dcross.at[i], cross_at[i])
    grads(down, own_at)


def attn_parts(pieces, line, prev, own, cross, bias, sections, chunk=384):
    slots = len(pieces)
    tok, part = pieces[0].shape[1:]
    nk = bias.shape[0]
    block = (sections, 2, tok // sections, HD)
    vm = pl.BlockSpec(memory_space=pltpu.VMEM)
    bf, f32 = jnp.bfloat16, jnp.float32
    return pl.pallas_call(
        functools.partial(attn_kernel, slots, chunk),
        out_shape=(
            jax.ShapeDtypeStruct((slots * part // HD // 2, nk, 2 * tok), bf),
            jax.ShapeDtypeStruct((HD, nk), bf),
            jax.ShapeDtypeStruct((LINE,) + block, f32),
            jax.ShapeDtypeStruct(block, f32),
            jax.ShapeDtypeStruct((LINE,) + block, bf),
        ),
        in_specs=[vm] * (slots + 5),
        out_specs=(vm,) * 5,
        scratch_shapes=[
            pltpu.VMEM((slots, 2, tok, part), bf),
            pltpu.VMEM((nk, HD), bf),
            pltpu.VMEM((nk, HD), bf),
            pltpu.VMEM((nk, HD), f32),
            pltpu.VMEM((nk, HD), f32),
            *[pltpu.VMEM((nk, 2 * tok), f32) for _ in range(4)],
        ],
        cost_estimate=pl.CostEstimate(
            flops=8 * slots * tok * part * nk,
            bytes_accessed=4 * 1024 * 1024,
            transcendentals=slots * tok * part // HD * nk,
        ),
        compiler_params=pltpu.CompilerParams(vmem_limit_bytes=24 * 1024 * 1024),
        name="attn_bwd",
    )(*pieces, line, prev, own, cross, bias)


def dq_kernel(slots, ds_ref, kt_ref, *refs):
    dq_out, dq_ref = refs[:slots], refs[slots]
    tok, part = dq_out[0].shape
    scale = HD ** (-0.5)

    def step(t, carry):
        for u in range(2):
            p = 2 * t + u
            dqt = jnp.dot(kt_ref[...], ds_ref[p], preferred_element_type=jnp.float32)
            dqq = (dqt.T * scale).astype(jnp.bfloat16)
            for o, (slot, n) in enumerate(head_places(p, part // HD)):
                dq_ref[slot, :, n] = dqq[o * tok : (o + 1) * tok]
        return carry

    lax.fori_loop(0, ds_ref.shape[0] // 2, step, 0)
    for s in range(slots):
        dq_out[s][...] = dq_ref[s]


def dq_parts(ds, kt, slots, tok, part):
    vm = pl.BlockSpec(memory_space=pltpu.VMEM)
    bf = jnp.bfloat16
    return pl.pallas_call(
        functools.partial(dq_kernel, slots),
        out_shape=tuple(jax.ShapeDtypeStruct((tok, part), bf) for _ in range(slots)),
        in_specs=[vm] * 2,
        out_specs=(vm,) * slots,
        scratch_shapes=[pltpu.VMEM((slots, tok, part), bf)],
        cost_estimate=pl.CostEstimate(
            flops=2 * ds.size * HD, bytes_accessed=2 * ds.size, transcendentals=0
        ),
        compiler_params=pltpu.CompilerParams(vmem_limit_bytes=12 * 1024 * 1024),
        name="attn_dq",
    )(ds, kt)


def join_kernel(sign, *refs):
    *pieces, out_ref, sems = refs
    count, part = len(pieces), pieces[0].shape[-1]
    head = lax.axis_index("x")
    copies = []
    for n, piece in enumerate(pieces):
        at = lax.rem(head + (count + sign * n) % count, count) * part
        copies.append(
            pltpu.make_async_copy(piece, out_ref.at[:, pl.ds(pl.multiple_of(at, HD), part)], sems.at[n])
        )
    for c in copies:
        c.start()
    for c in copies:
        c.wait()


def joined(pieces, sign):
    rows, part = pieces[0].shape
    vm = pl.BlockSpec(memory_space=pltpu.VMEM)
    return pl.pallas_call(
        functools.partial(join_kernel, sign),
        out_shape=jax.ShapeDtypeStruct((rows, len(pieces) * part), pieces[0].dtype),
        in_specs=[vm] * len(pieces),
        out_specs=pl.BlockSpec(memory_space=pl.ANY),
        scratch_shapes=[pltpu.SemaphoreType.DMA((len(pieces),))],
        compiler_params=pltpu.CompilerParams(vmem_limit_bytes=2 * 1024 * 1024),
        name="join_heads",
    )(*pieces)


def shifted(value, axis, steps, ring):
    count = lax.axis_size(axis)
    pairs = [(i, i + steps) for i in range(count)]
    pairs = [(i, j % count) for i, j in pairs if ring or 0 <= j < count]
    return lax.ppermute(value, axis, pairs)


def exchanged(value, axes):
    return lax.all_to_all(value, axes, 0, 0, tiled=True)


def chosen(which, options):
    out = options[0]
    for n, option in enumerate(options[1:], 1):
        out = jnp.where(which == n, option, out)
    return out


def body(queries, grad_out, keys_values, doc_ids):
    _, tok_rows, width = queries.shape
    kv_width = keys_values.shape[2]
    ring = lax.axis_size("x")
    part = width // ring
    core, chip, head = [lax.axis_index(a) for a in ("core", "z", "x")]
    place = (lax.axis_index("y") * LINE + chip) * 2 + core
    bf, f32 = jnp.bfloat16, jnp.float32
    chips = jnp.arange(LINE, dtype=jnp.int32).reshape(LINE, 1, 1, 1)

    def cut(arrays, k):
        at = lax.rem(head + k, ring) * part
        return jnp.stack([lax.dynamic_slice_in_dim(a[0], at, part, 1) for a in arrays])

    pieces = lax.optimization_barrier([cut((queries, grad_out), k) for k in range(ring)])
    own = chosen(head, jnp.split(keys_values, ring, axis=2))
    own = lax.optimization_barrier((own, pieces[1]))[0]
    prev = shifted(own, "y", 1, False)
    pieces[2] = shifted(pieces[2], "x", 2, True)
    for k in (1, 3):
        pieces[k] = shifted(pieces[k], "x", k, True)
    line = exchanged(jnp.where(chips > chip, own[None], prev[None]), "z")
    cross = jnp.where(chips == chip, jnp.where(core == 1, prev, own)[None], line)
    cross = shifted(cross, "core", 1, True)

    total = (2 * LINE + 1) * tok_rows
    first = place * tok_rows
    qdoc = lax.dynamic_slice_in_dim(doc_ids, first, tok_rows, 0)
    padded = jnp.concatenate([jnp.full((total - tok_rows,), -1, jnp.int32), doc_ids])
    kdoc = lax.dynamic_slice_in_dim(padded, first, total, 0)
    kat = jnp.arange(total, dtype=jnp.int32) - (total - tok_rows)
    qat = jnp.arange(tok_rows, dtype=jnp.int32)
    seen = (kat[:, None] <= qat[None, :]) & (kdoc[:, None] == qdoc[None, :])
    bias = jnp.where(seen, 0.0, -1e30).astype(f32)

    sections = lax.axis_size("h") * ring
    ds, kt, dline, down, dcross = attn_parts(pieces, line, prev, own, cross, bias, sections)

    arrived = shifted(dcross, "core", 1, True).astype(f32)
    chips = chips[..., None]
    dline = dline + jnp.where((chips != chip) | (core == 1), arrived, 0.0)
    later = shifted(jnp.where(chips >= chip, dline, 0.0).astype(bf), "y", -1, False)
    dq = dq_parts(ds, kt, ring, tok_rows, part)
    parts = [dq[0]] + [shifted(dq[k], "x", -k, True) for k in range(1, ring)]

    here = down[None] + jnp.where(core == 1, 0.0, arrived)
    later = later.astype(f32) + jnp.where(chips == chip, here, 0.0)
    grad = jnp.where(chips < chip, dline, later).astype(bf)
    rows = tok_rows // sections
    grad = exchanged(grad.reshape(LINE * sections, 2, rows, HD), ("z", "h", "x"))
    grad = grad.astype(f32).reshape(LINE * lax.axis_size("h"), ring, 2, rows, HD).sum(axis=0)
    grad_kv = grad.astype(bf).transpose(1, 2, 0, 3).reshape(2, rows, kv_width)
    grad_queries = joined(parts, 1).reshape(1, tok_rows, width)
    return (grad_queries, grad_kv)


def solution(mesh):
    names = ("y", "z", "core", "h", "x")
    fine = jax.sharding.Mesh(mesh.devices.reshape(-1, LINE, 2, 2, 4), names)
    ctx, section = names[:3], names[3:]
    return jax.shard_map(
        body,
        mesh=fine,
        in_specs=(P(section, ctx, None), P(section, ctx, None), P(None, ctx, None), P()),
        out_specs=(P(section, ctx, None), P(None, ctx + section, None)),
        check_vma=False,
    )
```
